256 devices in a mesh: rows: 256 (over y, x, z, core).
Axes of the slice: x: 4, y: 4, z: 8, core: 2. Of those that a mesh axis runs over, the one named last changes fastest.
Arguments:
- start_panel: float32 [8, 262144], P(None, 'rows'), may hold values from -10 to 10, as said below
- diagonal_inverse: bfloat16 [256, 1024, 1024], P('rows'), may hold values from -0.6 to 12.5
- right_factor: bfloat16 [256, 1024, 1024], P('rows'), may hold values from -0.03125 to 0.03125
- left_factor: bfloat16 [256, 1024, 1024], P('rows'), may hold values from -0.03125 to 0.03125
Outputs:
- new_panels: float32 [24, 262144], P(None, 'rows')
- coefficients: float32 [3, 32, 8], replicated
- first_coefficients: float32 [3, 32, 8], replicated
The draws below stay inside these ranges and needn't reach their ends.
Inputs may be any that keep to these rules, and one draw needn't show every extreme that they name: The rows of start_panel are orthonormal under the inner product divided by 262144, up to float32 rounding.
All inputs are finite; a program needn't handle non-finite values.
Results may differ from the reference program's by a relative error of at most 0.014.
Values sent between devices are 32-bit elements; how exact they have to be, the bound alone decides.
A program may use at most 64 MiB of HBM per device.

```python
import jax
import jax.numpy as jnp
from jax import lax

BLOCK = 1024
PANEL = 8
STEPS = 3
BASIS = 32
BLOCK_ROWS = 256
UNKNOWNS = 262144
LEVELS = 8


def draw_start_panel(key, part):
    split_keys = jax.random.split(jax.random.fold_in(key, 11), 3)
    noise_rows = jnp.clip(jax.random.normal(split_keys[0], (PANEL, UNKNOWNS), jnp.float32), -6.0, 6.0)
    weights = jax.random.uniform(split_keys[1], (PANEL,), jnp.float32, -0.35, 0.35)
    common = jnp.clip(jax.random.normal(split_keys[2], (UNKNOWNS,), jnp.float32), -6.0, 6.0)
    raw = noise_rows + weights[:, None] * common[None, :]
    gram = jnp.dot(raw, raw.T, precision=lax.Precision.HIGHEST) / UNKNOWNS
    lower = jnp.linalg.cholesky(gram)
    return jax.scipy.linalg.solve_triangular(lower, raw, lower=True)


def draw_diagonal_inverse(key, part):
    split_keys = jax.random.split(jax.random.fold_in(key, 23), 2)
    spread = 0.5 * BLOCK ** (-0.5)
    position = lax.broadcasted_iota(jnp.int32, (BLOCK_ROWS, 1), 0).astype(jnp.float32) / (BLOCK_ROWS - 1)
    offdiag = spread * jnp.clip(jax.random.normal(split_keys[0], (BLOCK_ROWS, BLOCK, BLOCK), jnp.float32), -6.0, 6.0)
    diagonal = (1.0 + 2.0 * position) * jnp.exp(jax.random.uniform(split_keys[1], (BLOCK_ROWS, BLOCK), jnp.float32, -0.4, 0.4))
    identity = (lax.broadcasted_iota(jnp.int32, (BLOCK, BLOCK), 0) == lax.broadcasted_iota(jnp.int32, (BLOCK, BLOCK), 1)).astype(jnp.float32)
    return (offdiag + identity[None, :, :] * diagonal[:, :, None]).astype(jnp.bfloat16)


def block_levels(own_key, extent, pieces, smallest, top_value):
    gain = 1.0
    for dim, shards_of in pieces:
        steps = jax.random.uniform(jax.random.fold_in(jax.random.fold_in(own_key, 6), dim), (shards_of,), jnp.float32, smallest / len(pieces), top_value / len(pieces))
        gain = gain * jnp.repeat(jnp.exp(steps), extent[dim] // shards_of).reshape((-1,) + (1,) * (len(extent) - 1 - dim))
    return gain


def bell_draw(rng, extent, scale, most, shards=(), kind=jnp.bfloat16):
    drawn = scale * jax.random.normal(rng, extent, jnp.float32)
    if shards:
        drawn = drawn * block_levels(rng, extent, shards, -0.22, 0.18)
    return jnp.clip(drawn, -most, most).astype(kind)


def setup_inputs(seed: int = 0) -> dict:
    keys = jax.random.split(jax.random.key(seed), 5)
    start_panel = draw_start_panel(jax.random.fold_in(keys[4], 71), 0)
    diagonal_inverse = draw_diagonal_inverse(jax.random.fold_in(keys[4], 71), 0)
    right_factor = bell_draw(keys[2], (BLOCK_ROWS, BLOCK, BLOCK), (32 * BLOCK) ** -0.5, 0.03125, ((0, 256),))
    left_factor = bell_draw(keys[3], (BLOCK_ROWS, BLOCK, BLOCK), (32 * BLOCK) ** -0.5, 0.03125, ((0, 256),))
    return dict(start_panel=start_panel, diagonal_inverse=diagonal_inverse, right_factor=right_factor, left_factor=left_factor)


epsilon = 1e-06

def apply_rows(matrices, vectors):

    def single(couple):
        matrix, vector = couple
        return jnp.dot(vector.astype(jnp.float32), matrix.astype(jnp.float32), preferred_element_type=jnp.float32)
    return lax.map(single, (matrices, vectors))

def cyclic_solve(current, diagonal_inverse, right_factor, left_factor):
    updated = current.reshape(PANEL, BLOCK_ROWS, BLOCK).transpose(1, 0, 2)
    for height in range(LEVELS):
        distance = 2 ** height
        lowered = updated.astype(jnp.bfloat16)
        upward = apply_rows(right_factor, lowered)
        downward = apply_rows(left_factor, lowered)
        padding = jnp.zeros((distance, PANEL, BLOCK), jnp.float32)
        from_below = jnp.concatenate([padding, upward[:BLOCK_ROWS - distance]], 0)
        from_above = jnp.concatenate([downward[distance:], padding], 0)
        updated = updated - from_below - from_above
    solved = apply_rows(diagonal_inverse, updated.astype(jnp.bfloat16))
    return solved.transpose(1, 0, 2).reshape(PANEL, UNKNOWNS)

def product(left, right):
    return jnp.dot(left, right, precision=lax.Precision.HIGHEST)

def reference(start_panel, diagonal_inverse, right_factor, left_factor):
    krylov_basis = start_panel
    current = start_panel
    produced = []
    coefficients = []
    firsts = []
    for iteration in range(STEPS):
        images = cyclic_solve(current, diagonal_inverse, right_factor, left_factor)
        height = krylov_basis.shape[0]
        coef_first = product(krylov_basis, images.T) / UNKNOWNS
        projected = images - product(coef_first.T, krylov_basis)
        coef_second = product(krylov_basis, projected.T) / UNKNOWNS
        remainder = projected - product(coef_second.T, krylov_basis)
        gram_new = product(remainder, remainder.T) / UNKNOWNS + epsilon * jnp.eye(PANEL, dtype=jnp.float32)
        lower_factor = jnp.linalg.cholesky(gram_new)
        fresh = jax.scipy.linalg.solve_triangular(lower_factor, remainder, lower=True)
        column_block = jnp.zeros((BASIS, PANEL), jnp.float32)
        column_block = column_block.at[:height].set(coef_first + coef_second)
        column_block = column_block.at[height:height + PANEL].set(lower_factor.T)
        first_block = jnp.zeros((BASIS, PANEL), jnp.float32).at[:height].set(coef_first)
        produced.append(fresh)
        coefficients.append(column_block)
        firsts.append(first_block)
        krylov_basis = jnp.concatenate([krylov_basis, fresh], 0)
        current = fresh
    return (jnp.concatenate(produced, 0), jnp.stack(coefficients), jnp.stack(firsts))
```

```python
import functools

import jax
import jax.numpy as jnp
from jax import lax
from jax.experimental import pallas as pl
from jax.experimental.pallas import tpu as pltpu
from jax.sharding import PartitionSpec as P

STEPS = 3
BASIS = 32
PANEL = 8
CHUNKS = 4
EPSILON = 1e-06
MESH = pl.DeviceIdType.MESH


def split(values):
    leading = values.astype(jnp.bfloat16).astype(jnp.float32)
    return jnp.concatenate([leading, values - leading], 0).astype(jnp.bfloat16)


def times(pair, matrix):
    both = jnp.dot(pair, matrix, preferred_element_type=jnp.float32)
    return both[:PANEL] + both[PANEL:]


def combine(weights, rows_ref):
    total = weights[:, 0:1] * rows_ref[0:1, :]
    for b in range(1, BASIS):
        total = total + weights[:, b : b + 1] * rows_ref[b : b + 1, :]
    return total


def kernel(
    n,
    group,
    hooks,
    start_hbm,
    diagonal_hbm,
    right_hbm,
    left_hbm,
    panels_ref,
    coefficients_ref,
    firsts_ref,
    factors,
    diagonal,
    state,
    outgoing,
    incoming,
    basis,
    images,
    mixing,
    gram,
    near_parts,
    far_parts,
    load_sems,
    send_sems,
    receive_sems,
    near_send,
    near_receive,
    far_send,
    far_receive,
):
    me = lax.axis_index("rows")
    columns = state.shape[1]
    width = columns // CHUNKS
    levels = n.bit_length() - 1
    unknowns = n * columns
    others = n // group
    spot = lax.rem(me, group)
    lane_start = me - spot
    plane = me // group

    def peer(offset):
        return lax.rem(me + (offset + n), n)

    loads = [
        pltpu.make_async_copy(right_hbm.at[0], factors.at[0], load_sems.at[0]),
        pltpu.make_async_copy(left_hbm.at[0], factors.at[1], load_sems.at[1]),
        pltpu.make_async_copy(start_hbm, state, load_sems.at[2]),
        pltpu.make_async_copy(diagonal_hbm.at[0], diagonal, load_sems.at[3]),
    ]
    for load in (loads[2], loads[0], loads[1], loads[3]):
        load.start()

    barrier = pltpu.get_barrier_semaphore()
    near = [lane_start + lax.rem(spot + k, group) for k in range(1, group)]
    far = [spot + group * lax.rem(plane + k, others) for k in range(1, others)]
    across = []
    distance = 1
    while distance < group:
        across += [peer(distance), peer(-distance)]
        distance *= 2
    for target in near + far + across:
        pl.semaphore_signal(barrier, inc=1, device_id=(target,), device_id_type=MESH)

    row8 = lax.broadcasted_iota(jnp.int32, (PANEL, BASIS), 0)
    lane8 = lax.broadcasted_iota(jnp.int32, (PANEL, BASIS), 1)
    basis[...] = jnp.zeros_like(basis)
    images[...] = jnp.zeros_like(images)
    mixing[...] = jnp.where(lane8 == row8, 1.0, 0.0)
    loads[2].wait()
    basis[PANEL : 2 * PANEL, :] = state[...]
    pl.semaphore_wait(barrier, len(near) + len(far) + len(across))
    loads[0].wait()
    loads[1].wait()

    def send(solve, level, chunk):
        slot = solve * levels + level
        parity = level % 2
        distance = 2**level
        last = level == levels - 1
        for way, offset in ((0, distance),) if last else ((0, distance), (1, -distance)):
            pltpu.make_async_remote_copy(
                src_ref=outgoing.at[parity, chunk, way],
                dst_ref=incoming.at[slot, chunk, way],
                send_sem=send_sems.at[parity],
                recv_sem=receive_sems.at[slot, chunk],
                device_id=(peer(offset),),
                device_id_type=MESH,
            ).start()

    def sent(level):
        parity = level % 2
        whole = outgoing.at[parity, :, 0] if level == levels - 1 else outgoing.at[parity]
        pltpu.make_async_copy(whole, whole, send_sems.at[parity]).wait()

    def received(solve, level, chunk):
        slot = solve * levels + level
        distance = 2**level
        place = slice(chunk * width, (chunk + 1) * width)
        if level == levels - 1:
            arrived = incoming.at[slot, chunk, 0]
        else:
            arrived = incoming.at[slot, chunk]
        pltpu.make_async_copy(arrived, arrived, receive_sems.at[slot, chunk]).wait()
        value = state[:, place]
        if level == levels - 1:
            value = value - incoming[slot, chunk, 0]
        else:
            value = value - jnp.where(me >= distance, incoming[slot, chunk, 0], 0.0)
            value = value - jnp.where(me < n - distance, incoming[slot, chunk, 1], 0.0)
        state[:, place] = value
        return value

    def place_of(chunk):
        return slice(chunk * width, (chunk + 1) * width)

    def first_level(solve):
        pair = split(state[...])
        for chunk in range(CHUNKS):
            for way in range(2):
                outgoing[0, chunk, way] = times(pair, factors[way, :, place_of(chunk)])
            send(solve, 0, chunk)

    def middle_level(solve, level):
        parity = level % 2
        totals = {}
        for part in range(CHUNKS):
            pair = split(received(solve, level - 1, part))
            for chunk in range(CHUNKS):
                for way in range(2):
                    term = times(pair, factors[way, place_of(part), place_of(chunk)])
                    key = (chunk, way)
                    totals[key] = totals[key] + term if part else term
                    if part == CHUNKS - 1:
                        outgoing[parity, chunk, way] = totals[key]
                if part == CHUNKS - 1:
                    send(solve, level, chunk)
        sent(level - 1)

    def last_level(solve):
        level = levels - 1
        parity = level % 2
        side = jnp.where(me >= n // 2, 1, 0)
        totals = {}
        for part in range(CHUNKS):
            pair = split(received(solve, level - 1, part))
            for chunk in range(CHUNKS):
                term = times(pair, factors[side, place_of(part), place_of(chunk)])
                totals[chunk] = totals[chunk] + term if part else term
                if part == CHUNKS - 1:
                    outgoing[parity, chunk, 0] = totals[chunk]
                    send(solve, level, chunk)
        sent(level - 1)

    def final_part(solve):
        total = None
        for part in range(CHUNKS):
            pair = split(received(solve, levels - 1, part))
            term = times(pair, diagonal[place_of(part), :])
            total = total + term if part else term
        sent(levels - 1)
        return total

    def near_start(step):
        local = lax.dot_general(
            basis[...],
            basis[...],
            (((1,), (1,)), ((), ())),
            precision=lax.Precision.HIGHEST,
            preferred_element_type=jnp.float32,
        ) * (1.0 / unknowns)
        for k in range(4):
            near_parts[step, spot, :, k * BASIS : (k + 1) * BASIS] = local[k * PANEL : (k + 1) * PANEL]
        mine = near_parts.at[step, spot]
        for target in near:
            pltpu.make_async_remote_copy(
                src_ref=mine,
                dst_ref=mine,
                send_sem=near_send.at[step],
                recv_sem=near_receive.at[step],
                device_id=(target,),
                device_id_type=MESH,
            ).start()

    def settle(parts, step, count, sem):
        some = parts.at[step, pl.ds(0, count)]
        pltpu.make_async_copy(some, some, sem.at[step]).wait()

    def far_start(step):
        settle(near_parts, step, group - 1, near_receive)
        far_parts[step, plane] = jnp.sum(near_parts[step], axis=0)
        mine = far_parts.at[step, plane]
        for target in far:
            pltpu.make_async_remote_copy(
                src_ref=mine,
                dst_ref=mine,
                send_sem=far_send.at[step],
                recv_sem=far_receive.at[step],
                device_id=(target,),
                device_id_type=MESH,
            ).start()
        settle(near_parts, step, group - 1, near_send)

    def expand(step):
        settle(far_parts, step, others - 1, far_receive)
        total = jnp.sum(far_parts[step], axis=0)
        for k in range(4):
            gram[k * PANEL : (k + 1) * PANEL, :] = total[:, k * BASIS : (k + 1) * BASIS]
        cross = gram[0:PANEL, :]
        rest = gram[PANEL:BASIS, :]
        through = jnp.zeros_like(cross)
        tall = jnp.zeros_like(rest)
        for k in range(PANEL, BASIS):
            through = through + cross[:, k : k + 1] * gram[k : k + 1, :]
            tall = tall + rest[:, k : k + 1] * gram[k : k + 1, :]
        both = 2.0 * cross - through
        tall = 2.0 * rest - tall
        again = jnp.zeros_like(cross)
        for k in range(PANEL, BASIS):
            again = again + both[:, k : k + 1] * gram[k : k + 1, :]
        left = cross - again
        square = cross - again
        for k in range(PANEL, BASIS):
            square = square - left[:, k : k + 1] * tall[k - PANEL : k - PANEL + 1, :]
        square = square + jnp.where(lane8 == row8, EPSILON, 0.0)
        mixed = jnp.where(lane8 < PANEL, jnp.where(lane8 == row8, 1.0, 0.0), -both)
        for k in range(PANEL):
            scale = lax.rsqrt(square[k : k + 1, k : k + 1])
            upper = square[k : k + 1, :] * scale
            mixed_row = mixed[k : k + 1, :] * scale
            column = square[:, k : k + 1] * scale
            square = jnp.where(row8 > k, square - column * upper, jnp.where(row8 == k, upper, square))
            mixed = jnp.where(row8 > k, mixed - column * mixed_row, jnp.where(row8 == k, mixed_row, mixed))
        upper = jnp.where(lane8 >= row8, square, 0.0)
        mixing[...] = mixed
        height = pl.multiple_of(PANEL * (step + 1), PANEL)
        zeros = jnp.zeros((PANEL, PANEL), jnp.float32)
        coefficients_ref[step, 0 : BASIS - PANEL, :] = tall[:, :PANEL]
        coefficients_ref[step, BASIS - PANEL : BASIS, :] = zeros
        coefficients_ref[step, pl.ds(height, PANEL), :] = upper[:, :PANEL]
        firsts_ref[step, 0 : BASIS - PANEL, :] = rest[:, :PANEL]
        firsts_ref[step, BASIS - PANEL : BASIS, :] = zeros
        fresh = combine(mixed, basis)
        panels_ref[pl.ds(pl.multiple_of(PANEL * step, PANEL), PANEL), :] = fresh
        settle(far_parts, step, others - 1, far_send)
        return fresh

    def after(solve, level):
        if level == hooks[0]:

            @pl.when(solve > 0)
            def _():
                near_start(solve - 1)

        if level == hooks[1]:

            @pl.when(solve > 0)
            def _():
                far_start(solve - 1)

        if level == hooks[2]:

            @pl.when(solve > 0)
            def _():
                fresh = expand(solve - 1)
                basis[pl.ds(pl.multiple_of(PANEL * (solve + 1), PANEL), PANEL), :] = fresh

    @pl.loop(0, STEPS)
    def _(solve):
        first_level(solve)
        after(solve, 0)
        for level in range(1, levels - 1):
            middle_level(solve, level)
            after(solve, level)
        last_level(solve)

        @pl.when(solve == 0)
        def _():
            loads[3].wait()

        images[0:PANEL, :] = final_part(solve)
        image = combine(mixing[...], images)
        state[...] = image
        basis[0:PANEL, :] = image
        images[pl.ds(pl.multiple_of(PANEL * (solve + 1), PANEL), PANEL), :] = image

    near_start(STEPS - 1)
    far_start(STEPS - 1)
    expand(STEPS - 1)


def arnoldi(n, group, hooks, start_panel, diagonal_inverse, right_factor, left_factor):
    columns = start_panel.shape[1]
    width = columns // CHUNKS
    levels = n.bit_length() - 1
    others = n // group
    vmem = pl.BlockSpec(memory_space=pltpu.VMEM)
    anywhere = pl.BlockSpec(memory_space=pl.ANY)
    dma = pltpu.SemaphoreType.DMA
    return pl.pallas_call(
        functools.partial(kernel, n, group, hooks),
        out_shape=(
            jax.ShapeDtypeStruct((STEPS * PANEL, columns), jnp.float32),
            jax.ShapeDtypeStruct((STEPS, BASIS, PANEL), jnp.float32),
            jax.ShapeDtypeStruct((STEPS, BASIS, PANEL), jnp.float32),
        ),
        in_specs=[anywhere] * 4,
        out_specs=(vmem, vmem, vmem),
        scratch_shapes=[
            pltpu.VMEM((2, columns, columns), jnp.bfloat16),
            pltpu.VMEM((columns, columns), jnp.bfloat16),
            pltpu.VMEM((PANEL, columns), jnp.float32),
            pltpu.VMEM((2, CHUNKS, 2, PANEL, width), jnp.float32),
            pltpu.VMEM((STEPS * levels, CHUNKS, 2, PANEL, width), jnp.float32),
            pltpu.VMEM((BASIS, columns), jnp.float32),
            pltpu.VMEM((BASIS, columns), jnp.float32),
            pltpu.VMEM((PANEL, BASIS), jnp.float32),
            pltpu.VMEM((BASIS, BASIS), jnp.float32),
            pltpu.VMEM((STEPS, group, PANEL, 4 * BASIS), jnp.float32),
            pltpu.VMEM((STEPS, others, PANEL, 4 * BASIS), jnp.float32),
            dma((4,)),
            dma((2,)),
            dma((STEPS * levels, CHUNKS)),
            dma((STEPS,)),
            dma((STEPS,)),
            dma((STEPS,)),
            dma((STEPS,)),
        ],
        compiler_params=pltpu.CompilerParams(
            collective_id=0, has_side_effects=True, vmem_limit_bytes=40 * 1024 * 1024
        ),
    )(start_panel, diagonal_inverse, right_factor, left_factor)


def solution(mesh):
    n = mesh.shape["rows"]
    group = 2 ** ((n.bit_length() - 1) // 2)
    hooks = (0, 2, 3) if n >= 64 else (0, 1, 2)
    placed = (P(None, "rows"), P("rows", None, None), P("rows", None, None), P("rows", None, None))
    return jax.shard_map(
        functools.partial(arnoldi, n, group, hooks),
        mesh=mesh,
        in_specs=placed,
        out_specs=(P(None, "rows"), P(), P()),
        check_vma=False,
    )
```

```python
import functools

import jax
import jax.numpy as jnp
from jax import lax
from jax.experimental import pallas as pl
from jax.experimental.pallas import tpu as pltpu
from jax.sharding import PartitionSpec as P

STEPS = 3
BASIS = 32
PANEL = 8
CUTS = (0, 512, 1024)
SPLITS = (CUTS,) * 8
EPSILON = 1e-06
VMEM_GRANT = 54 * 1024 * 1024
MESH = pl.DeviceIdType.MESH


def split(values):
    leading = values.astype(jnp.bfloat16).astype(jnp.float32)
    return jnp.concatenate([leading, values - leading], 0).astype(jnp.bfloat16)


def times(pair, matrix):
    both = jnp.dot(pair, matrix, preferred_element_type=jnp.float32)
    return both[:PANEL] + both[PANEL:]


def combine(weights, rows_ref):
    total = weights[:, 0:1] * rows_ref[0:1, :]
    for b in range(1, BASIS):
        total = total + weights[:, b : b + 1] * rows_ref[b : b + 1, :]
    return total


def kernel(
    n,
    group,
    hooks,
    start_hbm,
    diagonal_hbm,
    right_hbm,
    left_hbm,
    panels_ref,
    coefficients_ref,
    firsts_ref,
    factors,
    diagonal,
    state,
    outgoing,
    incoming,
    basis,
    images,
    mixing,
    gram,
    near_parts,
    far_parts,
    load_sems,
    send_sems,
    receive_sems,
    near_send,
    near_receive,
    far_send,
    far_receive,
):
    me = lax.axis_index("rows")
    columns = state.shape[1]
    levels = n.bit_length() - 1
    unknowns = n * columns
    others = n // group
    spot = lax.rem(me, group)
    lane_start = me - spot
    plane = me // group

    def peer(offset):
        return lax.rem(me + (offset + n), n)

    loads = [
        pltpu.make_async_copy(right_hbm.at[0], factors.at[0], load_sems.at[0]),
        pltpu.make_async_copy(left_hbm.at[0], factors.at[1], load_sems.at[1]),
        pltpu.make_async_copy(start_hbm, state, load_sems.at[2]),
        pltpu.make_async_copy(diagonal_hbm.at[0], diagonal, load_sems.at[3]),
    ]
    for load in (loads[2], loads[0], loads[1], loads[3]):
        load.start()

    barrier = pltpu.get_barrier_semaphore()
    near = [lane_start + lax.rem(spot + k, group) for k in range(1, group)]
    far = [spot + group * lax.rem(plane + k, others) for k in range(1, others)]
    for way, offset, sends, _ in ((0, 1, me < n - 1, None), (1, -1, me >= 1, None)):

        @pl.when(sends)
        def _():
            pl.semaphore_signal(barrier, inc=1, device_id=(peer(offset),), device_id_type=MESH)

    row8 = lax.broadcasted_iota(jnp.int32, (PANEL, BASIS), 0)
    lane8 = lax.broadcasted_iota(jnp.int32, (PANEL, BASIS), 1)
    basis[...] = jnp.zeros_like(basis)
    images[...] = jnp.zeros_like(images)
    mixing[...] = jnp.where(lane8 == row8, 1.0, 0.0)
    loads[2].wait()
    basis[PANEL : 2 * PANEL, :] = state[...]
    loads[0].wait()
    loads[1].wait()

    def place_of(level, chunk):
        return slice(*SPLITS[level][chunk : chunk + 2])

    def ways_of(level):
        distance = 2**level
        if level == levels - 1:
            return ((0, distance, None, None),)
        return (
            (0, distance, me < n - distance, me >= distance),
            (1, -distance, me >= distance, me < n - distance),
        )

    def where_needed(condition, action):
        if condition is None:
            action()
        else:
            pl.when(condition)(action)

    def send(solve, level, chunk):
        slot = solve * levels + level
        place = place_of(level, chunk)
        for way, offset, sends, _ in ways_of(level):
            copy = pltpu.make_async_remote_copy(
                src_ref=outgoing.at[level % 2, way, :, place],
                dst_ref=incoming.at[slot, way, :, place],
                send_sem=send_sems.at[level % 2, way],
                recv_sem=receive_sems.at[slot, chunk, way],
                device_id=(peer(offset),),
                device_id_type=MESH,
            )
            where_needed(sends, copy.start)

    def sent(level):
        for way, _, sends, _ in ways_of(level):
            whole = outgoing.at[level % 2, way]
            where_needed(sends, pltpu.make_async_copy(whole, whole, send_sems.at[level % 2, way]).wait)

    def received(solve, level, chunk):
        slot = solve * levels + level
        place = place_of(level, chunk)
        value = state[:, place]
        for way, _, _, takes in ways_of(level):
            arrived = incoming.at[slot, way, :, place]
            where_needed(takes, pltpu.make_async_copy(arrived, arrived, receive_sems.at[slot, chunk, way]).wait)
        for way, _, _, takes in ways_of(level):
            update = incoming[slot, way, :, place]
            value = value - (update if takes is None else jnp.where(takes, update, 0.0))
        state[:, place] = value
        return value

    def first_level(solve, entering):
        pair = split(state[...])
        for chunk in range(len(SPLITS[0]) - 1):
            for way in range(2):
                place = place_of(0, chunk)
                outgoing[0, way, :, place] = times(pair, factors[way, :, place])
            if entering:
                continue
            send(solve, 0, chunk)
        if entering:
            pl.semaphore_wait(barrier, jnp.where(me >= 1, 1, 0) + jnp.where(me < n - 1, 1, 0))
            for chunk in range(len(SPLITS[0]) - 1):
                send(solve, 0, chunk)

    def next_level(solve, level):
        parity = level % 2
        if level == levels - 1:
            sides = ((0, jnp.where(me >= n // 2, 1, 0)),)
        else:
            sides = ((0, 0), (1, 1))
        totals = {}
        parts = len(SPLITS[level - 1]) - 1
        for part in range(parts):
            pair = split(received(solve, level - 1, part))
            rows = place_of(level - 1, part)
            for chunk in range(len(SPLITS[level]) - 1):
                place = place_of(level, chunk)
                for way, side in sides:
                    term = times(pair, factors[side, rows, place])
                    totals[chunk, way] = totals[chunk, way] + term if part else term
                    if part == parts - 1:
                        outgoing[parity, way, :, place] = totals[chunk, way]
                if part == parts - 1:
                    send(solve, level, chunk)
        sent(level - 1)

    def final_part(solve):
        total = None
        for part in range(len(SPLITS[levels - 1]) - 1):
            pair = split(received(solve, levels - 1, part))
            term = times(pair, diagonal[place_of(levels - 1, part), :])
            total = total + term if part else term
        sent(levels - 1)
        return total

    def near_start(step):
        local = lax.dot_general(
            basis[...],
            basis[...],
            (((1,), (1,)), ((), ())),
            precision=lax.Precision.HIGHEST,
            preferred_element_type=jnp.float32,
        ) * (1.0 / unknowns)
        for k in range(4):
            near_parts[step, spot, :, k * BASIS : (k + 1) * BASIS] = local[k * PANEL : (k + 1) * PANEL]
        mine = near_parts.at[step, spot]
        for target in near:
            pltpu.make_async_remote_copy(
                src_ref=mine,
                dst_ref=mine,
                send_sem=near_send.at[step],
                recv_sem=near_receive.at[step],
                device_id=(target,),
                device_id_type=MESH,
            ).start()

    def settle(parts, step, count, sem):
        some = parts.at[step, pl.ds(0, count)]
        pltpu.make_async_copy(some, some, sem.at[step]).wait()

    def far_start(step):
        settle(near_parts, step, group - 1, near_receive)
        far_parts[step, plane] = jnp.sum(near_parts[step], axis=0)
        mine = far_parts.at[step, plane]
        for target in far:
            pltpu.make_async_remote_copy(
                src_ref=mine,
                dst_ref=mine,
                send_sem=far_send.at[step],
                recv_sem=far_receive.at[step],
                device_id=(target,),
                device_id_type=MESH,
            ).start()
        settle(near_parts, step, group - 1, near_send)

    def expand(step):
        settle(far_parts, step, others - 1, far_receive)
        total = jnp.sum(far_parts[step], axis=0)
        for k in range(4):
            gram[k * PANEL : (k + 1) * PANEL, :] = total[:, k * BASIS : (k + 1) * BASIS]
        cross = gram[0:PANEL, :]
        rest = gram[PANEL:BASIS, :]
        through = jnp.zeros_like(cross)
        tall = jnp.zeros_like(rest)
        for k in range(PANEL, BASIS):
            through = through + cross[:, k : k + 1] * gram[k : k + 1, :]
            tall = tall + rest[:, k : k + 1] * gram[k : k + 1, :]
        both = 2.0 * cross - through
        tall = 2.0 * rest - tall
        again = jnp.zeros_like(cross)
        for k in range(PANEL, BASIS):
            again = again + both[:, k : k + 1] * gram[k : k + 1, :]
        left = cross - again
        square = cross - again
        for k in range(PANEL, BASIS):
            square = square - left[:, k : k + 1] * tall[k - PANEL : k - PANEL + 1, :]
        square = square + jnp.where(lane8 == row8, EPSILON, 0.0)
        mixed = jnp.where(lane8 < PANEL, jnp.where(lane8 == row8, 1.0, 0.0), -both)
        lower = jnp.zeros_like(cross)
        for k in range(PANEL):
            scale = lax.rsqrt(square[k : k + 1, k : k + 1])
            upper = square[k : k + 1, :] * scale
            mixed_row = mixed[k : k + 1, :] * scale
            column = square[:, k : k + 1] * scale
            lower = jnp.where(lane8 % PANEL == k, jnp.where(row8 >= k, column, 0.0), lower)
            square = jnp.where(row8 > k, square - column * upper, jnp.where(row8 == k, upper, square))
            mixed = jnp.where(row8 > k, mixed - column * mixed_row, jnp.where(row8 == k, mixed_row, mixed))
        mixing[...] = mixed
        zeros = jnp.zeros((PANEL, PANEL), jnp.float32)
        here = lane8 // PANEL == step + 1
        coefficients_ref[step] = jnp.concatenate([both[:, PANEL:], zeros], 1) + jnp.where(here, lower, 0.0)
        firsts_ref[step] = jnp.concatenate([cross[:, PANEL:], zeros], 1)
        fresh = combine(mixed, basis)
        panels_ref[pl.ds(pl.multiple_of(PANEL * step, PANEL), PANEL), :] = fresh
        settle(far_parts, step, others - 1, far_send)
        return fresh

    def after(solve, level):
        if level == hooks[0]:

            @pl.when(solve > 0)
            def _():
                near_start(solve - 1)

        if level == hooks[1]:

            @pl.when(solve > 0)
            def _():
                far_start(solve - 1)

        if level == hooks[2]:

            @pl.when(solve > 0)
            def _():
                fresh = expand(solve - 1)
                basis[pl.ds(pl.multiple_of(PANEL * (solve + 1), PANEL), PANEL), :] = fresh

    first_level(0, True)

    @pl.loop(0, STEPS)
    def _(solve):
        @pl.when(solve > 0)
        def _():
            first_level(solve, False)

        after(solve, 0)
        for level in range(1, levels):
            next_level(solve, level)
            after(solve, level)

        @pl.when(solve == 0)
        def _():
            loads[3].wait()

        images[0:PANEL, :] = final_part(solve)
        image = combine(mixing[...], images)
        state[...] = image
        basis[0:PANEL, :] = image
        images[pl.ds(pl.multiple_of(PANEL * (solve + 1), PANEL), PANEL), :] = image

    near_start(STEPS - 1)
    far_start(STEPS - 1)
    expand(STEPS - 1)


def publish(panels_ref, coefficients_ref, firsts_ref, panels_out, coefficients_out, firsts_out):
    pairs = ((panels_ref, panels_out), (coefficients_ref, coefficients_out), (firsts_ref, firsts_out))
    for source, target in pairs:
        target[...] = source[...]


def arnoldi(n, group, hooks, start_panel, diagonal_inverse, right_factor, left_factor):
    columns = start_panel.shape[1]
    levels = n.bit_length() - 1
    others = n // group
    vmem = pl.BlockSpec(memory_space=pltpu.VMEM)
    anywhere = pl.BlockSpec(memory_space=pl.ANY)
    dma = pltpu.SemaphoreType.DMA
    shapes = (
        jax.ShapeDtypeStruct((STEPS * PANEL, columns), jnp.float32),
        jax.ShapeDtypeStruct((STEPS, PANEL, BASIS), jnp.float32),
        jax.ShapeDtypeStruct((STEPS, PANEL, BASIS), jnp.float32),
    )
    results = pl.pallas_call(
        functools.partial(kernel, n, group, hooks),
        out_shape=shapes,
        in_specs=[anywhere] * 4,
        out_specs=(vmem, vmem, vmem),
        scratch_shapes=[
            pltpu.VMEM((2, columns, columns), jnp.bfloat16),
            pltpu.VMEM((columns, columns), jnp.bfloat16),
            pltpu.VMEM((PANEL, columns), jnp.float32),
            pltpu.VMEM((2, 2, PANEL, columns), jnp.float32),
            pltpu.VMEM((STEPS * levels, 2, PANEL, columns), jnp.float32),
            pltpu.VMEM((BASIS, columns), jnp.float32),
            pltpu.VMEM((BASIS, columns), jnp.float32),
            pltpu.VMEM((PANEL, BASIS), jnp.float32),
            pltpu.VMEM((BASIS, BASIS), jnp.float32),
            pltpu.VMEM((STEPS, group, PANEL, 4 * BASIS), jnp.float32),
            pltpu.VMEM((STEPS, others, PANEL, 4 * BASIS), jnp.float32),
            dma((4,)),
            dma((2, 2)),
            dma((STEPS * levels, max(len(cuts) for cuts in SPLITS), 2)),
            dma((STEPS,)),
            dma((STEPS,)),
            dma((STEPS,)),
            dma((STEPS,)),
        ],
        compiler_params=pltpu.CompilerParams(
            collective_id=0, has_side_effects=True, vmem_limit_bytes=VMEM_GRANT
        ),
    )(start_panel, diagonal_inverse, right_factor, left_factor)
    panels, coefficients, firsts = pl.pallas_call(
        publish,
        out_shape=shapes,
        in_specs=[vmem] * 3,
        out_specs=(vmem,) * 3,
        name="publish",
    )(*results)
    return panels, jnp.swapaxes(coefficients, 1, 2), jnp.swapaxes(firsts, 1, 2)


def solution(mesh):
    n = mesh.shape["rows"]
    group = 2 ** ((n.bit_length() - 1) // 2)
    hooks = (0, 2, 3) if n >= 64 else (0, 1, 2)
    placed = (P(None, "rows"), P("rows", None, None), P("rows", None, None), P("rows", None, None))
    return jax.shard_map(
        functools.partial(arnoldi, n, group, hooks),
        mesh=mesh,
        in_specs=placed,
        out_specs=(P(None, "rows"), P(), P()),
        check_vma=False,
    )
```

```python
import functools

import jax
import jax.numpy as jnp
from jax import lax
from jax.experimental import pallas as pl
from jax.experimental.pallas import tpu as pltpu
from jax.sharding import PartitionSpec as P

STEPS = 3
BASIS = 32
PANEL = 8
HALVES = (0, 512, 1024)
QUARTERS = (0, 256, 512, 768, 1024)
SPLITS = (HALVES,) * 8
EPSILON = 1e-06
VMEM_GRANT = 53 * 1024 * 1024
MESH = pl.DeviceIdType.MESH


def split(values):
    leading = values.astype(jnp.bfloat16).astype(jnp.float32)
    return jnp.concatenate([leading, values - leading], 0).astype(jnp.bfloat16)


def times(pair, matrix):
    both = jnp.dot(pair, matrix, preferred_element_type=jnp.float32)
    return both[:PANEL] + both[PANEL:]


def combine(weights, rows_ref, start=0, stop=BASIS):
    total = weights[:, start : start + 1] * rows_ref[start : start + 1, :]
    for b in range(start + 1, stop):
        total = total + weights[:, b : b + 1] * rows_ref[b : b + 1, :]
    return total


def kernel(
    n,
    group,
    hooks,
    start_hbm,
    diagonal_hbm,
    right_hbm,
    left_hbm,
    panels_ref,
    coefficients_ref,
    firsts_ref,
    factors,
    diagonal,
    state,
    outgoing,
    incoming,
    basis,
    images,
    known,
    mixing,
    gram,
    near_parts,
    far_parts,
    load_sems,
    send_sems,
    receive_sems,
    near_send,
    near_receive,
    far_send,
    far_receive,
):
    me = lax.axis_index("rows")
    columns = state.shape[1]
    levels = n.bit_length() - 1
    unknowns = n * columns
    others = n // group
    spot = lax.rem(me, group)
    lane_start = me - spot
    plane = me // group

    def peer(offset):
        return lax.rem(me + (offset + n), n)

    load_start = pltpu.make_async_copy(start_hbm, state, load_sems.at[8])
    load_diagonal = pltpu.make_async_copy(diagonal_hbm.at[0], diagonal, load_sems.at[9])
    loads = []
    load_start.start()
    for chunk in range(len(SPLITS[0]) - 1):
        for way, factor in ((0, right_hbm), (1, left_hbm)):
            place = slice(*SPLITS[0][chunk : chunk + 2])
            load = pltpu.make_async_copy(factor.at[0, :, place], factors.at[way, :, place], load_sems.at[len(loads)])
            load.start()
            loads.append(load)
    load_diagonal.start()

    barrier = pltpu.get_barrier_semaphore()
    in_line = sorted(range(1, group), key=lambda k: -min(k, group - k))
    in_plane = sorted(range(1, others), key=lambda k: -min(k % 4, 4 - k % 4) - min(k // 4, 4 - k // 4))
    near = [spot + group * lax.rem(plane + k, others) for k in in_plane]
    far = [lane_start + lax.rem(spot + k, group) for k in in_line]
    for way, offset, sends, _ in ((0, 1, me < n - 1, None), (1, -1, me >= 1, None)):

        @pl.when(sends)
        def _():
            pl.semaphore_signal(barrier, inc=1, device_id=(peer(offset),), device_id_type=MESH)

    row8 = lax.broadcasted_iota(jnp.int32, (PANEL, BASIS), 0)
    lane8 = lax.broadcasted_iota(jnp.int32, (PANEL, BASIS), 1)
    basis[...] = jnp.zeros_like(basis)
    images[...] = jnp.zeros_like(images)
    known[...] = jnp.zeros_like(known)
    mixing[...] = jnp.where(lane8 == row8, 1.0, 0.0)
    load_start.wait()
    basis[PANEL : 2 * PANEL, :] = state[...]

    def place_of(level, chunk):
        return slice(*SPLITS[level][chunk : chunk + 2])

    def ways_of(level):
        distance = 2**level
        if level == levels - 1:
            return ((0, distance, None, None),)
        return (
            (0, distance, me < n - distance, me >= distance),
            (1, -distance, me >= distance, me < n - distance),
        )

    def urgent(level):
        distance = 2**level
        stretch = group if distance < group else group * 4
        return jnp.where(lax.rem(me, stretch) < distance, 1, 0)

    def where_needed(condition, action):
        if condition is None:
            action()
        else:
            pl.when(condition)(action)

    def send(solve, level, chunk, way):
        slot = solve * levels + level
        place = place_of(level, chunk)
        offset = 2**level if level == levels - 1 else 2**level * (1 - 2 * way)
        copy = pltpu.make_async_remote_copy(
            src_ref=outgoing.at[level % 2, way, :, place],
            dst_ref=incoming.at[slot, way, :, place],
            send_sem=send_sems.at[level % 2, way],
            recv_sem=receive_sems.at[slot, chunk, way],
            device_id=(peer(offset),),
            device_id_type=MESH,
        )
        if level == levels - 1:
            copy.start()
        else:
            pl.when(jnp.logical_and(me + offset >= 0, me + offset < n))(copy.start)

    def sent(level):
        for way, _, sends, _ in ways_of(level):
            whole = outgoing.at[level % 2, way]
            where_needed(sends, pltpu.make_async_copy(whole, whole, send_sems.at[level % 2, way]).wait)

    def received(solve, level, chunk):
        slot = solve * levels + level
        place = place_of(level, chunk)
        value = state[:, place]
        for way, _, _, takes in ways_of(level):
            arrived = incoming.at[slot, way, :, place]
            where_needed(takes, pltpu.make_async_copy(arrived, arrived, receive_sems.at[slot, chunk, way]).wait)
        for way, _, _, takes in ways_of(level):
            update = incoming[slot, way, :, place]
            value = value - (update if takes is None else jnp.where(takes, update, 0.0))
        state[:, place] = value
        return value

    def first_level(solve, entering):
        pair = split(state[...])
        first = 0 if entering else urgent(0)
        pieces = [(way, chunk) for chunk in range(len(SPLITS[0]) - 1) for way in (first, 1 - first)]
        for number, (way, chunk) in enumerate(pieces):
            place = place_of(0, chunk)
            if entering:
                loads[number].wait()
            outgoing[0, way, :, place] = times(pair, factors[way, :, place])
            if not entering:
                send(solve, 0, chunk, way)
        if entering:
            pl.semaphore_wait(barrier, jnp.where(me >= 1, 1, 0) + jnp.where(me < n - 1, 1, 0))
            for way, chunk in pieces:
                send(solve, 0, chunk, way)

    def next_level(solve, level):
        parity = level % 2
        first = urgent(level)
        if level == levels - 1:
            sides = ((0, jnp.where(me >= n // 2, 1, 0)),)
        else:
            sides = ((first, first), (1 - first, 1 - first))
        totals = {}
        parts = len(SPLITS[level - 1]) - 1
        for part in range(parts):
            pair = split(received(solve, level - 1, part))
            rows = place_of(level - 1, part)
            for chunk in range(len(SPLITS[level]) - 1):
                for number, (way, side) in enumerate(sides):
                    place = place_of(level, chunk)
                    term = times(pair, factors[side, rows, place])
                    totals[number, chunk] = totals[number, chunk] + term if part else term
                    if part == parts - 1:
                        outgoing[parity, way, :, place] = totals[number, chunk]
                        send(solve, level, chunk, way)
        sent(level - 1)

    def final_part(solve):
        total = None
        for part in range(len(SPLITS[levels - 1]) - 1):
            pair = split(received(solve, levels - 1, part))
            term = times(pair, diagonal[place_of(levels - 1, part), :])
            total = total + term if part else term
        sent(levels - 1)
        return total

    def near_start(step):
        local = lax.dot_general(
            basis[...],
            basis[...],
            (((1,), (1,)), ((), ())),
            precision=lax.Precision.HIGHEST,
            preferred_element_type=jnp.float32,
        ) * (1.0 / unknowns)
        for k in range(4):
            near_parts[step, plane, :, k * BASIS : (k + 1) * BASIS] = local[k * PANEL : (k + 1) * PANEL]
        mine = near_parts.at[step, plane]
        for target in near:
            pltpu.make_async_remote_copy(
                src_ref=mine,
                dst_ref=mine,
                send_sem=near_send.at[step],
                recv_sem=near_receive.at[step],
                device_id=(target,),
                device_id_type=MESH,
            ).start()

    def settle(parts, step, count, sem):
        some = parts.at[step, pl.ds(0, count)]
        pltpu.make_async_copy(some, some, sem.at[step]).wait()

    def far_start(step):
        settle(near_parts, step, others - 1, near_receive)
        far_parts[step, spot] = jnp.sum(near_parts[step], axis=0)
        mine = far_parts.at[step, spot]
        for target in far:
            pltpu.make_async_remote_copy(
                src_ref=mine,
                dst_ref=mine,
                send_sem=far_send.at[step],
                recv_sem=far_receive.at[step],
                device_id=(target,),
                device_id_type=MESH,
            ).start()
        settle(near_parts, step, others - 1, near_send)

    def expand(step):
        settle(far_parts, step, group - 1, far_receive)
        total = jnp.sum(far_parts[step], axis=0)
        for k in range(4):
            gram[k * PANEL : (k + 1) * PANEL, :] = total[:, k * BASIS : (k + 1) * BASIS]
        cross = gram[0:PANEL, :]
        rest = gram[PANEL:BASIS, :]
        through = jnp.zeros_like(cross)
        tall = jnp.zeros_like(rest)
        for k in range(PANEL, BASIS):
            through = through + cross[:, k : k + 1] * gram[k : k + 1, :]
            tall = tall + rest[:, k : k + 1] * gram[k : k + 1, :]
        both = 2.0 * cross - through
        tall = 2.0 * rest - tall
        again = jnp.zeros_like(cross)
        for k in range(PANEL, BASIS):
            again = again + both[:, k : k + 1] * gram[k : k + 1, :]
        left = cross - again
        square = cross - again
        for k in range(PANEL, BASIS):
            square = square - left[:, k : k + 1] * tall[k - PANEL : k - PANEL + 1, :]
        square = square + jnp.where(lane8 == row8, EPSILON, 0.0)
        mixed = jnp.where(lane8 < PANEL, jnp.where(lane8 == row8, 1.0, 0.0), -both)
        lower = jnp.zeros_like(cross)
        for k in range(PANEL):
            scale = lax.rsqrt(square[k : k + 1, k : k + 1])
            upper = square[k : k + 1, :] * scale
            mixed_row = mixed[k : k + 1, :] * scale
            column = square[:, k : k + 1] * scale
            lower = jnp.where(lane8 % PANEL == k, jnp.where(row8 >= k, column, 0.0), lower)
            square = jnp.where(row8 > k, square - column * upper, jnp.where(row8 == k, upper, square))
            mixed = jnp.where(row8 > k, mixed - column * mixed_row, jnp.where(row8 == k, mixed_row, mixed))
        mixing[...] = mixed
        zeros = jnp.zeros((PANEL, PANEL), jnp.float32)
        here = lane8 // PANEL == step + 1
        coefficients_ref[step] = jnp.concatenate([both[:, PANEL:], zeros], 1) + jnp.where(here, lower, 0.0)
        firsts_ref[step] = jnp.concatenate([cross[:, PANEL:], zeros], 1)
        fresh = combine(mixed, basis)
        panels_ref[pl.ds(pl.multiple_of(PANEL * step, PANEL), PANEL), :] = fresh
        settle(far_parts, step, group - 1, far_send)
        return fresh

    def after(solve, level):
        if level == hooks[0]:

            @pl.when(solve > 0)
            def _():
                near_start(solve - 1)

        if level == hooks[1]:

            @pl.when(solve > 0)
            def _():
                far_start(solve - 1)

        if level == hooks[2]:

            @pl.when(solve > 0)
            def _():
                fresh = expand(solve - 1)
                basis[pl.ds(pl.multiple_of(PANEL * (solve + 1), PANEL), PANEL), :] = fresh
                known[...] = combine(mixing[...], images, PANEL)

    first_level(0, True)

    @pl.loop(0, STEPS)
    def _(solve):
        @pl.when(solve > 0)
        def _():
            first_level(solve, False)

        after(solve, 0)
        for level in range(1, levels):
            next_level(solve, level)
            after(solve, level)

        @pl.when(solve == 0)
        def _():
            load_diagonal.wait()

        images[0:PANEL, :] = final_part(solve)
        image = combine(mixing[...], images, 0, PANEL) + known[...]
        state[...] = image
        basis[0:PANEL, :] = image
        images[pl.ds(pl.multiple_of(PANEL * (solve + 1), PANEL), PANEL), :] = image

    near_start(STEPS - 1)
    far_start(STEPS - 1)
    expand(STEPS - 1)


def publish(panels_ref, coefficients_ref, firsts_ref, panels_out, coefficients_out, firsts_out):
    pairs = ((panels_ref, panels_out), (coefficients_ref, coefficients_out), (firsts_ref, firsts_out))
    for source, target in pairs:
        target[...] = source[...]


def arnoldi(n, group, hooks, start_panel, diagonal_inverse, right_factor, left_factor):
    columns = start_panel.shape[1]
    levels = n.bit_length() - 1
    others = n // group
    vmem = pl.BlockSpec(memory_space=pltpu.VMEM)
    anywhere = pl.BlockSpec(memory_space=pl.ANY)
    dma = pltpu.SemaphoreType.DMA
    shapes = (
        jax.ShapeDtypeStruct((STEPS * PANEL, columns), jnp.float32),
        jax.ShapeDtypeStruct((STEPS, PANEL, BASIS), jnp.float32),
        jax.ShapeDtypeStruct((STEPS, PANEL, BASIS), jnp.float32),
    )
    results = pl.pallas_call(
        functools.partial(kernel, n, group, hooks),
        out_shape=shapes,
        in_specs=[anywhere] * 4,
        out_specs=(vmem, vmem, vmem),
        scratch_shapes=[
            pltpu.VMEM((2, columns, columns), jnp.bfloat16),
            pltpu.VMEM((columns, columns), jnp.bfloat16),
            pltpu.VMEM((PANEL, columns), jnp.float32),
            pltpu.VMEM((2, 2, PANEL, columns), jnp.float32),
            pltpu.VMEM((STEPS * levels, 2, PANEL, columns), jnp.float32),
            pltpu.VMEM((BASIS, columns), jnp.float32),
            pltpu.VMEM((BASIS, columns), jnp.float32),
            pltpu.VMEM((PANEL, columns), jnp.float32),
            pltpu.VMEM((PANEL, BASIS), jnp.float32),
            pltpu.VMEM((BASIS, BASIS), jnp.float32),
            pltpu.VMEM((STEPS, others, PANEL, 4 * BASIS), jnp.float32),
            pltpu.VMEM((STEPS, group, PANEL, 4 * BASIS), jnp.float32),
            dma((10,)),
            dma((2, 2)),
            dma((STEPS * levels, max(len(cuts) for cuts in SPLITS), 2)),
            dma((STEPS,)),
            dma((STEPS,)),
            dma((STEPS,)),
            dma((STEPS,)),
        ],
        compiler_params=pltpu.CompilerParams(
            collective_id=0, has_side_effects=True, vmem_limit_bytes=VMEM_GRANT
        ),
    )(start_panel, diagonal_inverse, right_factor, left_factor)
    panels, coefficients, firsts = pl.pallas_call(
        publish,
        out_shape=shapes,
        in_specs=[vmem] * 3,
        out_specs=(vmem,) * 3,
        name="publish",
        compiler_params=pltpu.CompilerParams(vmem_limit_bytes=1024 * 1024),
    )(*results)
    return panels, jnp.swapaxes(coefficients, 1, 2), jnp.swapaxes(firsts, 1, 2)


def solution(mesh):
    n = mesh.shape["rows"]
    group = 2 ** ((n.bit_length() - 1) // 2)
    hooks = (0, 4, 6) if n >= 64 else (0, 1, 2)
    placed = (P(None, "rows"), P("rows", None, None), P("rows", None, None), P("rows", None, None))
    return jax.shard_map(
        functools.partial(arnoldi, n, group, hooks),
        mesh=mesh,
        in_specs=placed,
        out_specs=(P(None, "rows"), P(), P()),
        check_vma=False,
    )
```

```python
import functools

import jax
import jax.numpy as jnp
from jax import lax
from jax.experimental import pallas as pl
from jax.experimental.pallas import tpu as pltpu
from jax.sharding import PartitionSpec as P

STEPS = 3
BASIS = 32
PANEL = 8
HALVES = (0, 512, 1024)
QUARTERS = (0, 256, 512, 768, 1024)
SPLITS = (HALVES,) * 8
EPSILON = 1e-06
VMEM_GRANT = 53 * 1024 * 1024
MESH = pl.DeviceIdType.MESH


def split(values):
    leading = values.astype(jnp.bfloat16).astype(jnp.float32)
    return jnp.concatenate([leading, values - leading], 0).astype(jnp.bfloat16)


def times(pair, matrix):
    both = jnp.dot(pair, matrix, preferred_element_type=jnp.float32)
    return both[:PANEL] + both[PANEL:]


def combine(weights, rows_ref, start=0, stop=BASIS):
    total = weights[:, start : start + 1] * rows_ref[start : start + 1, :]
    for b in range(start + 1, stop):
        total = total + weights[:, b : b + 1] * rows_ref[b : b + 1, :]
    return total


def kernel(
    n,
    group,
    hooks,
    start_hbm,
    diagonal_hbm,
    right_hbm,
    left_hbm,
    panels_ref,
    coefficients_ref,
    firsts_ref,
    factors,
    diagonal,
    state,
    outgoing,
    incoming,
    basis,
    images,
    known,
    mixing,
    gram,
    near_parts,
    far_parts,
    load_sems,
    send_sems,
    receive_sems,
    near_send,
    near_receive,
    far_send,
    far_receive,
):
    me = lax.axis_index("rows")
    columns = state.shape[1]
    levels = n.bit_length() - 1
    unknowns = n * columns
    others = n // group
    spot = lax.rem(me, group)
    lane_start = me - spot
    plane = me // group

    def peer(offset):
        return lax.rem(me + (offset + n), n)

    load_start = pltpu.make_async_copy(start_hbm, state, load_sems.at[8])
    load_diagonal = pltpu.make_async_copy(diagonal_hbm.at[0], diagonal, load_sems.at[9])
    loads = []
    load_start.start()
    for chunk in range(len(SPLITS[0]) - 1):
        for way, factor in ((0, right_hbm), (1, left_hbm)):
            place = slice(*SPLITS[0][chunk : chunk + 2])
            load = pltpu.make_async_copy(factor.at[0, :, place], factors.at[way, :, place], load_sems.at[len(loads)])
            load.start()
            loads.append(load)
    load_diagonal.start()

    barrier = pltpu.get_barrier_semaphore()
    in_line = sorted(range(1, group), key=lambda k: -min(k, group - k))
    in_plane = sorted(range(1, others), key=lambda k: -min(k % 4, 4 - k % 4) - min(k // 4, 4 - k // 4))
    near = [spot + group * lax.rem(plane + k, others) for k in in_plane]
    far = [lane_start + lax.rem(spot + k, group) for k in in_line]
    for way, offset, sends, _ in ((0, 1, me < n - 1, None), (1, -1, me >= 1, None)):

        @pl.when(sends)
        def _():
            pl.semaphore_signal(barrier, inc=1, device_id=(peer(offset),), device_id_type=MESH)

    row8 = lax.broadcasted_iota(jnp.int32, (PANEL, BASIS), 0)
    lane8 = lax.broadcasted_iota(jnp.int32, (PANEL, BASIS), 1)
    basis[...] = jnp.zeros_like(basis)
    images[...] = jnp.zeros_like(images)
    known[...] = jnp.zeros_like(known)
    mixing[...] = jnp.where(lane8 == row8, 1.0, 0.0)
    load_start.wait()
    basis[PANEL : 2 * PANEL, :] = state[...]

    def place_of(level, chunk):
        return slice(*SPLITS[level][chunk : chunk + 2])

    def ways_of(level):
        distance = 2**level
        if level == levels - 1:
            return ((0, distance, None, None),)
        return (
            (0, distance, me < n - distance, me >= distance),
            (1, -distance, me >= distance, me < n - distance),
        )

    def urgent(level):
        distance = 2**level
        stretch = group if distance < group else group * 4
        return jnp.where(lax.rem(me, stretch) < distance, 1, 0)

    def where_needed(condition, action):
        if condition is None:
            action()
        else:
            pl.when(condition)(action)

    def send(solve, level, chunk, way):
        slot = solve * levels + level
        place = place_of(level, chunk)
        offset = 2**level if level == levels - 1 else 2**level * (1 - 2 * way)
        copy = pltpu.make_async_remote_copy(
            src_ref=outgoing.at[level % 2, way, :, place],
            dst_ref=incoming.at[slot, way, :, place],
            send_sem=send_sems.at[level % 2, way],
            recv_sem=receive_sems.at[slot, chunk, way],
            device_id=(peer(offset),),
            device_id_type=MESH,
        )
        if level == levels - 1:
            copy.start()
        else:
            pl.when(jnp.logical_and(me + offset >= 0, me + offset < n))(copy.start)

    def sent(level):
        for way, _, sends, _ in ways_of(level):
            whole = outgoing.at[level % 2, way]
            where_needed(sends, pltpu.make_async_copy(whole, whole, send_sems.at[level % 2, way]).wait)

    def received(solve, level, chunk):
        slot = solve * levels + level
        place = place_of(level, chunk)
        value = state[:, place]
        for way, _, _, takes in ways_of(level):
            arrived = incoming.at[slot, way, :, place]
            where_needed(takes, pltpu.make_async_copy(arrived, arrived, receive_sems.at[slot, chunk, way]).wait)
        for way, _, _, takes in ways_of(level):
            update = incoming[slot, way, :, place]
            value = value - (update if takes is None else jnp.where(takes, update, 0.0))
        state[:, place] = value
        return value

    def first_level(solve, entering):
        pair = split(state[...])
        first = 0 if entering else urgent(0)
        pieces = [(way, chunk) for chunk in range(len(SPLITS[0]) - 1) for way in (first, 1 - first)]
        for number, (way, chunk) in enumerate(pieces):
            place = place_of(0, chunk)
            if entering:
                loads[number].wait()
            outgoing[0, way, :, place] = times(pair, factors[way, :, place])
            if not entering:
                send(solve, 0, chunk, way)
        if entering:
            pl.semaphore_wait(barrier, jnp.where(me >= 1, 1, 0) + jnp.where(me < n - 1, 1, 0))
            for way, chunk in pieces:
                send(solve, 0, chunk, way)

    def next_level(solve, level):
        parity = level % 2
        first = urgent(level)
        if level == levels - 1:
            sides = ((0, jnp.where(me >= n // 2, 1, 0)),)
        else:
            sides = ((first, first), (1 - first, 1 - first))
        totals = {}
        parts = len(SPLITS[level - 1]) - 1
        for part in range(parts):
            pair = split(received(solve, level - 1, part))
            rows = place_of(level - 1, part)
            for chunk in range(len(SPLITS[level]) - 1):
                for number, (way, side) in enumerate(sides):
                    place = place_of(level, chunk)
                    term = times(pair, factors[side, rows, place])
                    totals[number, chunk] = totals[number, chunk] + term if part else term
                    if part == parts - 1:
                        outgoing[parity, way, :, place] = totals[number, chunk]
                        send(solve, level, chunk, way)
        sent(level - 1)

    def final_part(solve):
        total = None
        for part in range(len(SPLITS[levels - 1]) - 1):
            pair = split(received(solve, levels - 1, part))
            term = times(pair, diagonal[place_of(levels - 1, part), :])
            total = total + term if part else term
        sent(levels - 1)
        return total

    def near_start(step):
        local = lax.dot_general(
            basis[...],
            basis[...],
            (((1,), (1,)), ((), ())),
            precision=lax.Precision.HIGHEST,
            preferred_element_type=jnp.float32,
        ) * (1.0 / unknowns)
        for k in range(4):
            near_parts[step, plane, :, k * BASIS : (k + 1) * BASIS] = local[k * PANEL : (k + 1) * PANEL]
        mine = near_parts.at[step, plane]
        for target in near:
            pltpu.make_async_remote_copy(
                src_ref=mine,
                dst_ref=mine,
                send_sem=near_send.at[step],
                recv_sem=near_receive.at[step],
                device_id=(target,),
                device_id_type=MESH,
            ).start()

    def settle(parts, step, count, sem):
        some = parts.at[step, pl.ds(0, count)]
        pltpu.make_async_copy(some, some, sem.at[step]).wait()

    def far_start(step):
        settle(near_parts, step, others - 1, near_receive)
        far_parts[step, spot] = jnp.sum(near_parts[step], axis=0)
        mine = far_parts.at[step, spot]
        for target in far:
            pltpu.make_async_remote_copy(
                src_ref=mine,
                dst_ref=mine,
                send_sem=far_send.at[step],
                recv_sem=far_receive.at[step],
                device_id=(target,),
                device_id_type=MESH,
            ).start()
        settle(near_parts, step, others - 1, near_send)

    def expand(step):
        settle(far_parts, step, group - 1, far_receive)
        total = jnp.sum(far_parts[step], axis=0)
        for k in range(4):
            gram[k * PANEL : (k + 1) * PANEL, :] = total[:, k * BASIS : (k + 1) * BASIS]
        cross = gram[0:PANEL, :]
        rest = gram[PANEL:BASIS, :]
        through = jnp.zeros_like(cross)
        tall = jnp.zeros_like(rest)
        for k in range(PANEL, BASIS):
            through = through + cross[:, k : k + 1] * gram[k : k + 1, :]
            tall = tall + rest[:, k : k + 1] * gram[k : k + 1, :]
        both = 2.0 * cross - through
        tall = 2.0 * rest - tall
        again = jnp.zeros_like(cross)
        for k in range(PANEL, BASIS):
            again = again + both[:, k : k + 1] * gram[k : k + 1, :]
        left = cross - again
        square = cross - again
        for k in range(PANEL, BASIS):
            square = square - left[:, k : k + 1] * tall[k - PANEL : k - PANEL + 1, :]
        square = square + jnp.where(lane8 == row8, EPSILON, 0.0)
        mixed = jnp.where(lane8 < PANEL, jnp.where(lane8 == row8, 1.0, 0.0), -both)
        lower = jnp.zeros_like(cross)
        for k in range(PANEL):
            scale = lax.rsqrt(square[k : k + 1, k : k + 1])
            upper = square[k : k + 1, :] * scale
            mixed_row = mixed[k : k + 1, :] * scale
            column = square[:, k : k + 1] * scale
            lower = jnp.where(lane8 % PANEL == k, jnp.where(row8 >= k, column, 0.0), lower)
            square = jnp.where(row8 > k, square - column * upper, jnp.where(row8 == k, upper, square))
            mixed = jnp.where(row8 > k, mixed - column * mixed_row, jnp.where(row8 == k, mixed_row, mixed))
        mixing[...] = mixed
        zeros = jnp.zeros((PANEL, PANEL), jnp.float32)
        here = lane8 // PANEL == step + 1
        coefficients_ref[step] = jnp.concatenate([both[:, PANEL:], zeros], 1) + jnp.where(here, lower, 0.0)
        firsts_ref[step] = jnp.concatenate([cross[:, PANEL:], zeros], 1)
        fresh = combine(mixed, basis)
        panels_ref[pl.ds(pl.multiple_of(PANEL * step, PANEL), PANEL), :] = fresh
        settle(far_parts, step, group - 1, far_send)
        return fresh

    def after(solve, level):
        if level == hooks[0]:

            @pl.when(solve > 0)
            def _():
                near_start(solve - 1)

        if level == hooks[1]:

            @pl.when(solve > 0)
            def _():
                far_start(solve - 1)

        if level == hooks[2]:

            @pl.when(solve > 0)
            def _():
                fresh = expand(solve - 1)
                basis[pl.ds(pl.multiple_of(PANEL * (solve + 1), PANEL), PANEL), :] = fresh
                known[...] = combine(mixing[...], images, PANEL)

    first_level(0, True)

    @pl.loop(0, STEPS)
    def _(solve):
        @pl.when(solve > 0)
        def _():
            first_level(solve, False)

        after(solve, 0)
        for level in range(1, levels):
            next_level(solve, level)
            after(solve, level)

        @pl.when(solve == 0)
        def _():
            load_diagonal.wait()

        images[0:PANEL, :] = final_part(solve)
        image = combine(mixing[...], images, 0, PANEL) + known[...]
        state[...] = image
        basis[0:PANEL, :] = image
        images[pl.ds(pl.multiple_of(PANEL * (solve + 1), PANEL), PANEL), :] = image

    near_start(STEPS - 1)
    far_start(STEPS - 1)
    expand(STEPS - 1)


def publish(panels_ref, coefficients_ref, firsts_ref, panels_out, coefficients_out, firsts_out):
    pairs = ((panels_ref, panels_out), (coefficients_ref, coefficients_out), (firsts_ref, firsts_out))
    for source, target in pairs:
        target[...] = source[...]


def arnoldi(n, group, hooks, start_panel, diagonal_inverse, right_factor, left_factor):
    columns = start_panel.shape[1]
    levels = n.bit_length() - 1
    others = n // group
    vmem = pl.BlockSpec(memory_space=pltpu.VMEM)
    anywhere = pl.BlockSpec(memory_space=pl.ANY)
    dma = pltpu.SemaphoreType.DMA
    shapes = (
        jax.ShapeDtypeStruct((STEPS * PANEL, columns), jnp.float32),
        jax.ShapeDtypeStruct((STEPS, PANEL, BASIS), jnp.float32),
        jax.ShapeDtypeStruct((STEPS, PANEL, BASIS), jnp.float32),
    )
    results = pl.pallas_call(
        functools.partial(kernel, n, group, hooks),
        out_shape=shapes,
        in_specs=[anywhere] * 4,
        out_specs=(vmem, vmem, vmem),
        scratch_shapes=[
            pltpu.VMEM((2, columns, columns), jnp.bfloat16),
            pltpu.VMEM((columns, columns), jnp.bfloat16),
            pltpu.VMEM((PANEL, columns), jnp.float32),
            pltpu.VMEM((2, 2, PANEL, columns), jnp.float32),
            pltpu.VMEM((STEPS * levels, 2, PANEL, columns), jnp.float32),
            pltpu.VMEM((BASIS, columns), jnp.float32),
            pltpu.VMEM((BASIS, columns), jnp.float32),
            pltpu.VMEM((PANEL, columns), jnp.float32),
            pltpu.VMEM((PANEL, BASIS), jnp.float32),
            pltpu.VMEM((BASIS, BASIS), jnp.float32),
            pltpu.VMEM((STEPS, others, PANEL, 4 * BASIS), jnp.float32),
            pltpu.VMEM((STEPS, group, PANEL, 4 * BASIS), jnp.float32),
            dma((10,)),
            dma((2, 2)),
            dma((STEPS * levels, max(len(cuts) for cuts in SPLITS), 2)),
            dma((STEPS,)),
            dma((STEPS,)),
            dma((STEPS,)),
            dma((STEPS,)),
        ],
        compiler_params=pltpu.CompilerParams(
            collective_id=0, has_side_effects=True, vmem_limit_bytes=VMEM_GRANT
        ),
    )(start_panel, diagonal_inverse, right_factor, left_factor)
    panels, coefficients, firsts = pl.pallas_call(
        publish,
        out_shape=shapes,
        in_specs=[vmem] * 3,
        out_specs=(vmem,) * 3,
        name="publish",
        compiler_params=pltpu.CompilerParams(vmem_limit_bytes=1024 * 1024),
    )(*results)
    return panels, jnp.swapaxes(coefficients, 1, 2), jnp.swapaxes(firsts, 1, 2)


def solution(mesh):
    n = mesh.shape["rows"]
    group = 2 ** ((n.bit_length() - 1) // 2)
    hooks = (1, 4, 6) if n >= 64 else (0, 1, 2)
    placed = (P(None, "rows"), P("rows", None, None), P("rows", None, None), P("rows", None, None))
    return jax.shard_map(
        functools.partial(arnoldi, n, group, hooks),
        mesh=mesh,
        in_specs=placed,
        out_specs=(P(None, "rows"), P(), P()),
        check_vma=False,
    )
```

```python
import functools

import jax
import jax.numpy as jnp
from jax import lax
from jax.experimental import pallas as pl
from jax.experimental.pallas import tpu as pltpu
from jax.sharding import PartitionSpec as P

STEPS = 3
BASIS = 32
PANEL = 8
HALVES = (0, 512, 1024)
QUARTERS = (0, 256, 512, 768, 1024)
SPLITS = (HALVES,) * 8
EPSILON = 1e-06
VMEM_GRANT = 53 * 1024 * 1024
MESH = pl.DeviceIdType.MESH


def split(values):
    leading = values.astype(jnp.bfloat16).astype(jnp.float32)
    return jnp.concatenate([leading, values - leading], 0).astype(jnp.bfloat16)


def times(pair, matrix):
    both = jnp.dot(pair, matrix, preferred_element_type=jnp.float32)
    return both[:PANEL] + both[PANEL:]


def in_quarters(terms):
    sums = list(terms[:4])
    for i, term in enumerate(terms[4:]):
        sums[i % 4] = sums[i % 4] + term
    return (sums[0] + sums[1]) + (sums[2] + sums[3])


def combine(weights, rows_ref, start=0, stop=BASIS):
    return in_quarters([weights[:, b : b + 1] * rows_ref[b : b + 1, :] for b in range(start, stop)])


def kernel(
    n,
    group,
    hooks,
    start_hbm,
    diagonal_hbm,
    right_hbm,
    left_hbm,
    panels_ref,
    coefficients_ref,
    firsts_ref,
    factors,
    diagonal,
    state,
    outgoing,
    incoming,
    basis,
    images,
    known,
    mixing,
    gram,
    near_parts,
    far_parts,
    load_sems,
    send_sems,
    receive_sems,
    near_send,
    near_receive,
    far_send,
    far_receive,
):
    me = lax.axis_index("rows")
    columns = state.shape[1]
    levels = n.bit_length() - 1
    unknowns = n * columns
    others = n // group
    spot = lax.rem(me, group)
    lane_start = me - spot
    plane = me // group

    def peer(offset):
        return lax.rem(me + (offset + n), n)

    load_start = pltpu.make_async_copy(start_hbm, state, load_sems.at[8])
    load_diagonal = pltpu.make_async_copy(diagonal_hbm.at[0], diagonal, load_sems.at[9])
    loads = []
    load_start.start()
    for chunk in range(len(SPLITS[0]) - 1):
        for way, factor in ((0, right_hbm), (1, left_hbm)):
            place = slice(*SPLITS[0][chunk : chunk + 2])
            load = pltpu.make_async_copy(factor.at[0, :, place], factors.at[way, :, place], load_sems.at[len(loads)])
            load.start()
            loads.append(load)
    load_diagonal.start()

    barrier = pltpu.get_barrier_semaphore()
    in_line = sorted(range(1, group), key=lambda k: -min(k, group - k))
    in_plane = sorted(range(1, others), key=lambda k: -min(k % 4, 4 - k % 4) - min(k // 4, 4 - k // 4))
    near = [spot + group * lax.rem(plane + k, others) for k in in_plane]
    far = [lane_start + lax.rem(spot + k, group) for k in in_line]
    for way, offset, sends, _ in ((0, 1, me < n - 1, None), (1, -1, me >= 1, None)):

        @pl.when(sends)
        def _():
            pl.semaphore_signal(barrier, inc=1, device_id=(peer(offset),), device_id_type=MESH)

    row8 = lax.broadcasted_iota(jnp.int32, (PANEL, BASIS), 0)
    lane8 = lax.broadcasted_iota(jnp.int32, (PANEL, BASIS), 1)
    basis[...] = jnp.zeros_like(basis)
    images[...] = jnp.zeros_like(images)
    known[...] = jnp.zeros_like(known)
    mixing[...] = jnp.where(lane8 == row8, 1.0, 0.0)
    load_start.wait()
    basis[PANEL : 2 * PANEL, :] = state[...]

    def place_of(level, chunk):
        return slice(*SPLITS[level][chunk : chunk + 2])

    def ways_of(level):
        distance = 2**level
        if level == levels - 1:
            return ((0, distance, None, None),)
        return (
            (0, distance, me < n - distance, me >= distance),
            (1, -distance, me >= distance, me < n - distance),
        )

    def urgent(level):
        distance = 2**level
        stretch = group if distance < group else group * 4
        return jnp.where(lax.rem(me, stretch) < distance, 1, 0)

    def where_needed(condition, action):
        if condition is None:
            action()
        else:
            pl.when(condition)(action)

    def send(solve, level, chunk, way):
        slot = solve * levels + level
        place = place_of(level, chunk)
        offset = 2**level if level == levels - 1 else 2**level * (1 - 2 * way)
        copy = pltpu.make_async_remote_copy(
            src_ref=outgoing.at[level % 2, way, :, place],
            dst_ref=incoming.at[slot, way, :, place],
            send_sem=send_sems.at[level % 2, way],
            recv_sem=receive_sems.at[slot, chunk, way],
            device_id=(peer(offset),),
            device_id_type=MESH,
        )
        if level == levels - 1:
            copy.start()
        else:
            pl.when(jnp.logical_and(me + offset >= 0, me + offset < n))(copy.start)

    def sent(level):
        for way, _, sends, _ in ways_of(level):
            whole = outgoing.at[level % 2, way]
            where_needed(sends, pltpu.make_async_copy(whole, whole, send_sems.at[level % 2, way]).wait)

    def received(solve, level, chunk):
        slot = solve * levels + level
        place = place_of(level, chunk)
        value = state[:, place]
        for way, _, _, takes in ways_of(level):
            arrived = incoming.at[slot, way, :, place]
            where_needed(takes, pltpu.make_async_copy(arrived, arrived, receive_sems.at[slot, chunk, way]).wait)
        for way, _, _, takes in ways_of(level):
            update = incoming[slot, way, :, place]
            value = value - (update if takes is None else jnp.where(takes, update, 0.0))
        state[:, place] = value
        return value

    def first_level(solve, entering):
        pair = split(state[...])
        first = 0 if entering else urgent(0)
        pieces = [(way, chunk) for chunk in range(len(SPLITS[0]) - 1) for way in (first, 1 - first)]
        for number, (way, chunk) in enumerate(pieces):
            place = place_of(0, chunk)
            if entering:
                loads[number].wait()
            outgoing[0, way, :, place] = times(pair, factors[way, :, place])
            if not entering:
                send(solve, 0, chunk, way)
        if entering:
            pl.semaphore_wait(barrier, jnp.where(me >= 1, 1, 0) + jnp.where(me < n - 1, 1, 0))
            for way, chunk in pieces:
                send(solve, 0, chunk, way)

    def next_level(solve, level):
        parity = level % 2
        first = urgent(level)
        if level == levels - 1:
            sides = ((0, jnp.where(me >= n // 2, 1, 0)),)
        else:
            sides = ((first, first), (1 - first, 1 - first))
        totals = {}
        parts = len(SPLITS[level - 1]) - 1
        for part in range(parts):
            pair = split(received(solve, level - 1, part))
            rows = place_of(level - 1, part)
            for chunk in range(len(SPLITS[level]) - 1):
                for number, (way, side) in enumerate(sides):
                    place = place_of(level, chunk)
                    term = times(pair, factors[side, rows, place])
                    totals[number, chunk] = totals[number, chunk] + term if part else term
                    if part == parts - 1:
                        outgoing[parity, way, :, place] = totals[number, chunk]
                        send(solve, level, chunk, way)
        sent(level - 1)

    def final_part(solve):
        total = None
        for part in range(len(SPLITS[levels - 1]) - 1):
            pair = split(received(solve, levels - 1, part))
            term = times(pair, diagonal[place_of(levels - 1, part), :])
            total = total + term if part else term
        sent(levels - 1)
        return total

    def near_start(step):
        local = lax.dot_general(
            basis[...],
            basis[...],
            (((1,), (1,)), ((), ())),
            precision=lax.Precision.HIGHEST,
            preferred_element_type=jnp.float32,
        ) * (1.0 / unknowns)
        for k in range(4):
            near_parts[step, plane, :, k * BASIS : (k + 1) * BASIS] = local[k * PANEL : (k + 1) * PANEL]
        mine = near_parts.at[step, plane]
        for target in near:
            pltpu.make_async_remote_copy(
                src_ref=mine,
                dst_ref=mine,
                send_sem=near_send.at[step],
                recv_sem=near_receive.at[step],
                device_id=(target,),
                device_id_type=MESH,
            ).start()

    def settle(parts, step, count, sem):
        some = parts.at[step, pl.ds(0, count)]
        pltpu.make_async_copy(some, some, sem.at[step]).wait()

    def far_start(step):
        settle(near_parts, step, others - 1, near_receive)
        far_parts[step, spot] = jnp.sum(near_parts[step], axis=0)
        mine = far_parts.at[step, spot]
        for target in far:
            pltpu.make_async_remote_copy(
                src_ref=mine,
                dst_ref=mine,
                send_sem=far_send.at[step],
                recv_sem=far_receive.at[step],
                device_id=(target,),
                device_id_type=MESH,
            ).start()
        settle(near_parts, step, others - 1, near_send)

    def expand(step):
        settle(far_parts, step, group - 1, far_receive)
        total = jnp.sum(far_parts[step], axis=0)
        for k in range(4):
            gram[k * PANEL : (k + 1) * PANEL, :] = total[:, k * BASIS : (k + 1) * BASIS]
        cross = gram[0:PANEL, :]
        rest = gram[PANEL:BASIS, :]
        span = range(PANEL, BASIS)
        through = in_quarters([cross[:, k : k + 1] * gram[k : k + 1, :] for k in span])
        tall = 2.0 * rest - in_quarters([rest[:, k : k + 1] * gram[k : k + 1, :] for k in span])
        both = 2.0 * cross - through
        left = cross - in_quarters([both[:, k : k + 1] * gram[k : k + 1, :] for k in span])
        square = left - in_quarters([left[:, k : k + 1] * tall[k - PANEL : k - PANEL + 1, :] for k in span])
        square = square + jnp.where(lane8 == row8, EPSILON, 0.0)
        mixed = jnp.where(lane8 < PANEL, jnp.where(lane8 == row8, 1.0, 0.0), -both)
        lower = jnp.zeros_like(cross)
        for k in range(PANEL):
            scale = lax.rsqrt(square[k : k + 1, k : k + 1])
            upper = square[k : k + 1, :] * scale
            mixed_row = mixed[k : k + 1, :] * scale
            column = square[:, k : k + 1] * scale
            lower = jnp.where(lane8 % PANEL == k, jnp.where(row8 >= k, column, 0.0), lower)
            square = jnp.where(row8 > k, square - column * upper, jnp.where(row8 == k, upper, square))
            mixed = jnp.where(row8 > k, mixed - column * mixed_row, jnp.where(row8 == k, mixed_row, mixed))
        mixing[...] = mixed
        zeros = jnp.zeros((PANEL, PANEL), jnp.float32)
        here = lane8 // PANEL == step + 1
        coefficients_ref[step] = jnp.concatenate([both[:, PANEL:], zeros], 1) + jnp.where(here, lower, 0.0)
        firsts_ref[step] = jnp.concatenate([cross[:, PANEL:], zeros], 1)
        fresh = combine(mixed, basis)
        panels_ref[pl.ds(pl.multiple_of(PANEL * step, PANEL), PANEL), :] = fresh
        settle(far_parts, step, group - 1, far_send)
        return fresh

    def after(solve, level):
        if level == hooks[0]:

            @pl.when(solve > 0)
            def _():
                near_start(solve - 1)

        if level == hooks[1]:

            @pl.when(solve > 0)
            def _():
                far_start(solve - 1)

        if level == hooks[2]:

            @pl.when(solve > 0)
            def _():
                fresh = expand(solve - 1)
                basis[pl.ds(pl.multiple_of(PANEL * (solve + 1), PANEL), PANEL), :] = fresh
                known[...] = combine(mixing[...], images, PANEL)

    first_level(0, True)

    @pl.loop(0, STEPS)
    def _(solve):
        @pl.when(solve > 0)
        def _():
            first_level(solve, False)

        after(solve, 0)
        for level in range(1, levels):
            next_level(solve, level)
            after(solve, level)

        @pl.when(solve == 0)
        def _():
            load_diagonal.wait()

        images[0:PANEL, :] = final_part(solve)
        image = combine(mixing[...], images, 0, PANEL) + known[...]
        state[...] = image
        basis[0:PANEL, :] = image
        images[pl.ds(pl.multiple_of(PANEL * (solve + 1), PANEL), PANEL), :] = image

    near_start(STEPS - 1)
    far_start(STEPS - 1)
    expand(STEPS - 1)


def publish(panels_ref, coefficients_ref, firsts_ref, panels_out, coefficients_out, firsts_out):
    pairs = ((panels_ref, panels_out), (coefficients_ref, coefficients_out), (firsts_ref, firsts_out))
    for source, target in pairs:
        target[...] = source[...]


def arnoldi(n, group, hooks, start_panel, diagonal_inverse, right_factor, left_factor):
    columns = start_panel.shape[1]
    levels = n.bit_length() - 1
    others = n // group
    vmem = pl.BlockSpec(memory_space=pltpu.VMEM)
    anywhere = pl.BlockSpec(memory_space=pl.ANY)
    dma = pltpu.SemaphoreType.DMA
    shapes = (
        jax.ShapeDtypeStruct((STEPS * PANEL, columns), jnp.float32),
        jax.ShapeDtypeStruct((STEPS, PANEL, BASIS), jnp.float32),
        jax.ShapeDtypeStruct((STEPS, PANEL, BASIS), jnp.float32),
    )
    results = pl.pallas_call(
        functools.partial(kernel, n, group, hooks),
        out_shape=shapes,
        in_specs=[anywhere] * 4,
        out_specs=(vmem, vmem, vmem),
        scratch_shapes=[
            pltpu.VMEM((2, columns, columns), jnp.bfloat16),
            pltpu.VMEM((columns, columns), jnp.bfloat16),
            pltpu.VMEM((PANEL, columns), jnp.float32),
            pltpu.VMEM((2, 2, PANEL, columns), jnp.float32),
            pltpu.VMEM((STEPS * levels, 2, PANEL, columns), jnp.float32),
            pltpu.VMEM((BASIS, columns), jnp.float32),
            pltpu.VMEM((BASIS, columns), jnp.float32),
            pltpu.VMEM((PANEL, columns), jnp.float32),
            pltpu.VMEM((PANEL, BASIS), jnp.float32),
            pltpu.VMEM((BASIS, BASIS), jnp.float32),
            pltpu.VMEM((STEPS, others, PANEL, 4 * BASIS), jnp.float32),
            pltpu.VMEM((STEPS, group, PANEL, 4 * BASIS), jnp.float32),
            dma((10,)),
            dma((2, 2)),
            dma((STEPS * levels, max(len(cuts) for cuts in SPLITS), 2)),
            dma((STEPS,)),
            dma((STEPS,)),
            dma((STEPS,)),
            dma((STEPS,)),
        ],
        compiler_params=pltpu.CompilerParams(
            collective_id=0, has_side_effects=True, vmem_limit_bytes=VMEM_GRANT
        ),
    )(start_panel, diagonal_inverse, right_factor, left_factor)
    panels, coefficients, firsts = pl.pallas_call(
        publish,
        out_shape=shapes,
        in_specs=[vmem] * 3,
        out_specs=(vmem,) * 3,
        name="publish",
        compiler_params=pltpu.CompilerParams(vmem_limit_bytes=1024 * 1024),
    )(*results)
    return panels, jnp.swapaxes(coefficients, 1, 2), jnp.swapaxes(firsts, 1, 2)


def solution(mesh):
    n = mesh.shape["rows"]
    group = 2 ** ((n.bit_length() - 1) // 2)
    hooks = (1, 4, 6) if n >= 64 else (0, 1, 2)
    placed = (P(None, "rows"), P("rows", None, None), P("rows", None, None), P("rows", None, None))
    return jax.shard_map(
        functools.partial(arnoldi, n, group, hooks),
        mesh=mesh,
        in_specs=placed,
        out_specs=(P(None, "rows"), P(), P()),
        check_vma=False,
    )
```
